512 devices in a mesh: grp: 2 (over y), seq: 32 (over z), head: 4 (over x), batch: 2 (over core).
Axes of the slice: x: 4, y: 2, z: 32, core: 2. Of those that a mesh axis runs over, the one named last changes fastest.
The devices are a block of a 4x8x32 slice.
Arguments:
- queries: bfloat16 [64, 64, 128], P(('grp', 'batch'), 'head'), parts along dimension 0, may hold values from -8 to 8
- key_cache: bfloat16 [64, 8, 8192, 128], P(('grp', 'batch'), 'head', 'seq'), parts along dimension 0, may hold values from -5 to 5
- value_cache: bfloat16 [64, 8, 8192, 128], P(('grp', 'batch'), 'head', 'seq'), parts along dimension 0, may hold values from -5 to 5
- gate_logits: float32 [2, 64, 64], P(None, ('grp', 'batch'), 'head'), parts along dimension 1, may hold values from -6 to 6
- lengths: int32 [64], P(('grp', 'batch')), parts along dimension 0, may hold values from 2048 to 8192, as said below
- chosen: int32 [64, 8, 16], P(('grp', 'batch'), 'head'), parts along dimension 0, may hold values from 0 to 63, as said below
- counts: int32 [64, 8], P(('grp', 'batch'), 'head'), parts along dimension 0, may hold values from 1 to 16, as said below
Outputs:
- output: bfloat16 [64, 64, 128], P(('grp', 'batch'), 'head'), parts along dimension 0
The draws below stay inside these ranges and needn't reach their ends.
There are 2 independent parts, one for each index of `grp`. The reference program is written for one: setup_inputs(seed, part) draws one part's arguments, and reference() takes and returns one part's arrays. A program takes and returns all parts, laid end to end along the dimension named above; each array names one. Nothing has to cross between parts.
Inputs may be any that keep to these rules, and one draw needn't show every extreme that they name: `lengths`: every draw has a sequence of the full length 8192. `chosen`: for each sequence and key-value head the first counts entries are distinct blocks that start below the sequence's length, and the first entry is block 0; the entries after them are ignored. `counts`: every draw has a sequence with 16 valid entries for every key-value head.
All inputs are finite; a program needn't handle non-finite values.
Results may differ from the reference program's by a relative error of at most 0.02.
Values may be sent and summed in bfloat16 or wider, within the bound.
A program may use at most 64 MiB of HBM per device.

```python
import math
import jax
import jax.numpy as jnp
from jax import lax

D_HEAD = 128
Q_HEADS = 64
KV_HEADS = 8
BLOCK = 128
SEQS = 32
BLOCKS = 64
CTX = 8192
TOPK = 16


def plan_draw(key):
    key_lengths = jax.random.fold_in(key, 11)
    key_scores = jax.random.fold_in(key, 12)
    key_counts = jax.random.fold_in(key, 13)
    key_longest = jax.random.fold_in(key, 14)
    lengths = jax.random.randint(key_lengths, (SEQS,), TOPK * BLOCK, CTX + 1, dtype=jnp.int32)
    longest = jax.random.randint(key_longest, (), 0, SEQS, dtype=jnp.int32)
    seq_ids = jnp.arange(SEQS, dtype=jnp.int32)
    lengths = jnp.where(seq_ids == longest, CTX, lengths).astype(jnp.int32)
    valid_blocks = (lengths + BLOCK - 1) // BLOCK
    block_ids = jnp.arange(BLOCKS, dtype=jnp.int32)
    raw_scores = jax.random.randint(key_scores, (SEQS, KV_HEADS, BLOCKS), 0, 1 << 16, dtype=jnp.int32)
    block_score = raw_scores * BLOCKS + block_ids[None, None, :]
    block_score = jnp.where(block_ids[None, None, :] < valid_blocks[:, None, None], block_score, -1 - block_ids[None, None, :])
    block_score = jnp.where(block_ids[None, None, :] == 0, 1 << 29, block_score)
    chosen = lax.top_k(block_score, TOPK)[1].astype(jnp.int32)
    counts = jax.random.randint(key_counts, (SEQS, KV_HEADS), 1, TOPK + 1, dtype=jnp.int32)
    counts = jnp.where((seq_ids == longest)[:, None], TOPK, counts).astype(jnp.int32)
    return (lengths, chosen, counts)


def draw_lengths(key, part):
    return plan_draw(key)[0]


def draw_chosen(key, part):
    return plan_draw(key)[1]


def draw_counts(key, part):
    return plan_draw(key)[2]


def draw_queries(key, part):
    full_shape = (SEQS, Q_HEADS, D_HEAD)
    drawn = jnp.clip(2.5 * jax.random.normal(jax.random.fold_in(key, 42), full_shape, jnp.float32), -8.0, 8.0)
    return drawn.astype(jnp.bfloat16)


def draw_key_cache(key, part):
    first_shape = (SEQS, KV_HEADS, BLOCK, D_HEAD)
    rest_shape = (SEQS, KV_HEADS, CTX - BLOCK, D_HEAD)
    first_rows = jnp.clip(jax.random.normal(jax.random.fold_in(key, 34), first_shape, jnp.float32), -5.0, 5.0)
    rest_rows = jnp.clip(jax.random.normal(jax.random.fold_in(key, 35), rest_shape, jnp.float32), -5.0, 5.0)
    return jnp.concatenate([first_rows, rest_rows], axis=2).astype(jnp.bfloat16)


def steps_of(key, extent, shards, low, top_value):
    loudness, own = 1.0, jax.random.fold_in(key, 6)
    for dim, blocks in shards:
        draws = jnp.exp(jax.random.uniform(jax.random.fold_in(own, dim), (blocks,), jnp.float32, low / len(shards), top_value / len(shards)))
        loudness = loudness * jnp.repeat(draws, extent[dim] // blocks).reshape([-1 if axis == dim else 1 for axis in range(len(extent))])
    return loudness


def noise(rng, dims, scale, limit, pieces=(), held_as=jnp.bfloat16):
    values = jax.random.normal(rng, dims, jnp.float32) * scale
    if len(pieces) > 0:
        values = steps_of(rng, dims, pieces, -0.22, 0.18) * values
    return jnp.clip(values, min=-limit, max=limit).astype(held_as)


def setup_inputs(seed: int = 0, part: int = 0) -> dict:
    key_list = jax.random.split(jax.random.key(seed), 8)
    part_splits = jax.random.split(jax.random.fold_in(key_list[7], part), 8)
    return {
        "queries": draw_queries(jax.random.fold_in(jax.random.fold_in(key_list[7], part), 71), part),
        "key_cache": draw_key_cache(jax.random.fold_in(jax.random.fold_in(key_list[7], part), 71), part),
        "value_cache": noise(part_splits[2], (SEQS, KV_HEADS, CTX, D_HEAD), 1.0, 5.0, ((0, 2), (1, 4), (2, 32))),
        "gate_logits": noise(part_splits[3], (2, SEQS, Q_HEADS), 1.5, 6.0, ((1, 2), (2, 4)), jnp.float32),
        "lengths": draw_lengths(jax.random.fold_in(jax.random.fold_in(key_list[7], part), 71), part),
        "chosen": draw_chosen(jax.random.fold_in(jax.random.fold_in(key_list[7], part), 71), part),
        "counts": draw_counts(jax.random.fold_in(jax.random.fold_in(key_list[7], part), 71), part),
    }


def attend(query_rows, key_rows, value_rows, live_mask, score_scale):
    scores = jnp.einsum('hgd,hnd->hgn', query_rows, key_rows, precision=lax.Precision.HIGHEST) * score_scale
    scores = jnp.where(live_mask[:, None, :], scores, -1e+30)
    row_max = lax.optimization_barrier(jnp.max(scores, axis=2, keepdims=True))
    weights = jnp.where(live_mask[:, None, :], jnp.exp(scores - row_max), 0.0)
    weight_sum = lax.optimization_barrier(jnp.sum(weights, axis=2, keepdims=True))
    rounded = lax.optimization_barrier(weights.astype(jnp.bfloat16)).astype(jnp.float32)
    summed = jnp.einsum('hgn,hnd->hgd', rounded, value_rows, precision=lax.Precision.HIGHEST)
    return summed / weight_sum

def pool_rows(rows_float, head_count, block_count, head_width, root_fill):
    summed = lax.optimization_barrier(jnp.sum(rows_float.reshape(head_count, block_count, BLOCK, head_width), axis=2)) / root_fill
    return lax.optimization_barrier(summed.astype(jnp.bfloat16)).astype(jnp.float32)

def one_sequence(sequence):
    query_in, key_rows, value_rows, gate_row, length, chosen_row, live_slots = sequence
    head_count, context, head_width = key_rows.shape
    group_size = query_in.shape[0] // head_count
    block_count = context // BLOCK
    score_scale = 1.0 / math.sqrt(head_width)
    query_rows = query_in.reshape(head_count, group_size, head_width).astype(jnp.float32)
    position = jnp.arange(context, dtype=jnp.int32)
    live_mask = position < length
    key_float = jnp.where(live_mask[None, :, None], key_rows.astype(jnp.float32), 0.0)
    value_float = jnp.where(live_mask[None, :, None], value_rows.astype(jnp.float32), 0.0)
    starts = jnp.arange(block_count, dtype=jnp.int32) * BLOCK
    filled = jnp.clip(length - starts, 0, BLOCK)
    root_fill = jnp.sqrt(jnp.maximum(filled, 1).astype(jnp.float32))[None, :, None]
    pooled_keys = pool_rows(key_float, head_count, block_count, head_width, root_fill)
    pooled_values = pool_rows(value_float, head_count, block_count, head_width, root_fill)
    block_live = jnp.broadcast_to((filled > 0)[None, :], (head_count, block_count))
    compressed = attend(query_rows, pooled_keys, pooled_values, block_live, score_scale)
    slot_live = jnp.arange(chosen_row.shape[1], dtype=jnp.int32)[None, :] < live_slots[:, None]
    block_ids = jnp.arange(block_count, dtype=jnp.int32)
    picked = jnp.any((chosen_row[:, :, None] == block_ids[None, None, :]) & slot_live[:, :, None], axis=1)
    token_mask = live_mask[None, :] & jnp.repeat(picked, BLOCK, axis=1)
    selected = attend(query_rows, key_float, value_float, token_mask, score_scale)
    gate_pair = jax.nn.sigmoid(gate_row).reshape(2, head_count, group_size, 1)
    mixed = gate_pair[0] * compressed + gate_pair[1] * selected
    return mixed.reshape(head_count * group_size, head_width).astype(jnp.bfloat16)

def reference(queries, key_cache, value_cache, gate_logits, lengths, chosen, counts):
    gate_rows = jnp.moveaxis(gate_logits, 0, 1)
    return lax.map(one_sequence, (queries, key_cache, value_cache, gate_rows, lengths, chosen, counts))
```

```python
import functools
import math

import jax
import jax.numpy as jnp
from jax import lax
from jax.experimental import pallas as pl
from jax.experimental.pallas import tpu as pltpu
from jax.sharding import PartitionSpec as P

BLOCK = 128
STRIDE = 4
NEAR = (-1, 1, 2)
CHUNK = 4
PIECE = 32
NEG = -1e30
MESH = pl.DeviceIdType.MESH


def iota(shape, dim):
    return lax.broadcasted_iota(jnp.int32, shape, dim)


def split_logs(logs):
    lane = iota(logs.shape, 1)
    spread = jnp.where(
        lane < PIECE,
        logs,
        jnp.where(lane < 2 * PIECE, pltpu.roll(logs, PIECE, 1), pltpu.roll(logs, 2 * PIECE, 1)),
    )
    high = spread.astype(jnp.bfloat16).astype(jnp.float32)
    rest = spread - high
    middle = rest.astype(jnp.bfloat16).astype(jnp.float32)
    low = rest - middle
    return jnp.where(lane < PIECE, high, jnp.where(lane < 2 * PIECE, middle, low)).astype(jnp.bfloat16)


def join_logs(pieces):
    pieces = pieces.astype(jnp.float32)
    width = pieces.shape[1]
    return (pieces + pltpu.roll(pieces, width - PIECE, 1)) + pltpu.roll(pieces, width - 2 * PIECE, 1)


def column(tile, lane):
    return jnp.broadcast_to(tile[:, lane : lane + 1], tile.shape)


def kernel(
    n,
    q_ref,
    k_hbm,
    v_hbm,
    gate_ref,
    length_ref,
    chosen_ref,
    count_ref,
    out_ref,
    k_buf,
    v_buf,
    sent,
    landed,
    board,
    gate_pad,
    gates,
    k_sem,
    v_sem,
    a_send,
    a_recv,
    b_send,
    b_recv,
):
    me = lax.axis_index("seq")
    sign = 1 - 2 * lax.axis_index("batch")
    rows, heads, context, width = k_buf.shape
    group = q_ref.shape[1] // heads
    local = context // BLOCK
    window = rows
    half = window // 2
    sources = n // window
    tile = heads * group
    scale = 1.0 / math.sqrt(width)

    def at(offset):
        return lax.rem(me + sign * offset + 2 * n, n)

    def remote(src, dst, send, recv, target):
        return pltpu.make_async_remote_copy(
            src_ref=src,
            dst_ref=dst,
            send_sem=send,
            recv_sem=recv,
            device_id={"seq": target},
            device_id_type=MESH,
        )

    barrier = pltpu.get_barrier_semaphore()
    for distance in range(half, 0, -1):
        for offset in (-distance, distance):
            pl.semaphore_signal(barrier, inc=1, device_id={"seq": at(offset)}, device_id_type=MESH)

    def loads(c):
        part = pl.ds(c * CHUNK, CHUNK)
        return (
            pltpu.make_async_copy(k_hbm.at[part], k_buf.at[part], k_sem.at[c]),
            pltpu.make_async_copy(v_hbm.at[part], v_buf.at[part], v_sem.at[c]),
        )

    for c in range(rows // CHUNK):
        for copy in loads(c):
            copy.start()

    gate_pad[...] = jnp.zeros_like(gate_pad)
    for branch in range(2):
        logits = gate_ref[branch]
        gate_pad[branch * rows : (branch + 1) * rows, : heads * group] = 1.0 / (1.0 + jnp.exp(-logits))
    turned = gate_pad[...].T
    lane = iota((group, width), 1)
    for b in range(rows):
        packed = jnp.zeros((group, width), jnp.float32)
        for branch in range(2):
            for h in range(heads):
                c = branch * heads + h
                here = turned[h * group : (h + 1) * group]
                moved = pltpu.roll(here, (c - (1 - branch) * rows - b) % width, 1)
                packed = jnp.where(lane == c, moved, packed)
        gates[b] = packed

    slot = iota((1, chosen_ref.shape[2]), 1)
    first = me * local

    def one_pair(b, h, live, root):
        scores = lax.dot_general(
            q_ref[b], k_buf[b, h], (((1,), (1,)), ((), ())), preferred_element_type=jnp.float32
        )[h * group : (h + 1) * group] * scale
        parts = [scores[:, j * BLOCK : (j + 1) * BLOCK] for j in range(local)]
        chosen = chosen_ref[b, h : h + 1, :]
        listed = slot < count_ref[h, b]
        masks = []
        for j in range(local):
            hit = jnp.where((chosen == first + j) & listed, 1.0, 0.0)
            picked = jnp.max(hit, axis=1, keepdims=True)
            masks.append(live[j] & (jnp.broadcast_to(picked, (group, BLOCK)) > 0.5))
        kept = [jnp.where(m, s, NEG) for m, s in zip(masks, parts)]
        top = jnp.max(functools.reduce(jnp.maximum, kept), axis=1, keepdims=True)
        weights = [jnp.where(m, jnp.exp(s - top), 0.0) for m, s in zip(masks, kept)]
        total = jnp.sum(sum(weights), axis=1, keepdims=True)
        pooled = [
            jnp.where(
                live[j][:, :1],
                jnp.sum(jnp.where(live[j], parts[j], 0.0), axis=1, keepdims=True) * root[j],
                NEG,
            )
            for j in range(local)
        ]
        pool_top = functools.reduce(jnp.maximum, pooled)
        pool_weights = [jnp.where(live[j][:, :1], jnp.exp(pooled[j] - pool_top), 0.0) for j in range(local)]
        pool_total = sum(pool_weights)
        spread = [jnp.where(live[j], pool_weights[j] * root[j], 0.0) for j in range(local)]
        left = jnp.concatenate(
            [jnp.concatenate(weights, axis=1), jnp.concatenate(spread, axis=1)], axis=0
        ).astype(jnp.bfloat16)
        summed = jnp.dot(left, v_buf[b, h], preferred_element_type=jnp.float32)
        result = []
        for top_of, total_of, value in (
            (top, total, summed[:group]),
            (pool_top, pool_total, summed[group:]),
        ):
            some = total_of > 0.0
            safe = jnp.where(some, total_of, 1.0)
            result.append((value / safe, jnp.where(some, top_of + jnp.log(safe), NEG)))
        return result

    def one_row(b):
        length = length_ref[b]
        live, root = [], []
        for j in range(local):
            start = (first + j) * BLOCK
            live.append(start + iota((group, BLOCK), 1) < length)
            filled = jnp.clip(length - start, 1, BLOCK).astype(jnp.float32)
            root.append(1.0 / jnp.sqrt(jnp.full((group, 1), filled, jnp.float32)))
        pairs = [one_pair(b, h, live, root) for h in range(heads)]
        logs = jnp.zeros((group, width), jnp.float32)
        for branch in range(2):
            values = jnp.concatenate([pairs[h][branch][0] for h in range(heads)], axis=0)
            sent[b, branch * tile : (branch + 1) * tile] = values.astype(jnp.bfloat16)
            for h in range(heads):
                logs = jnp.where(lane == branch * heads + h, pairs[h][branch][1], logs)
        sent[b, 2 * tile :] = split_logs(logs)

    def one_chunk(c, carry):
        for copy in loads(c):
            copy.wait()
        for i in range(CHUNK):
            one_row(c * CHUNK + i)
        return carry

    lax.fori_loop(0, rows // CHUNK, one_chunk, 0)

    pl.semaphore_wait(barrier, 2 * half)
    offsets = [d for d in range(-half, half) if d != 0]
    first_copies = []
    for i, offset in enumerate(sorted(offsets, key=lambda d: -abs(d))):
        target = at(offset)
        copy = remote(
            sent.at[lax.rem(target, window)],
            landed.at[offset + half],
            a_send.at[i],
            a_recv.at[offset + half],
            target,
        )
        copy.start()
        first_copies.append(copy)
    for copy in first_copies:
        copy.wait_recv()

    mine = lax.rem(me, window)
    logs = [
        join_logs(sent[mine, 2 * tile :] if d == 0 else landed[d + half, 2 * tile :])
        for d in range(-half, half)
    ]
    top = functools.reduce(jnp.maximum, logs)
    shares = [jnp.exp(x - top) for x in logs]
    total = functools.reduce(jnp.add, shares)
    merged = [jnp.zeros((group, width), jnp.float32) for _ in range(2 * heads)]
    inverse = 1.0 / total
    for share, d in zip(shares, range(-half, half)):
        share = share * inverse
        for c in range(0, 2 * heads, heads):
            part = pl.ds(c * group, tile)
            values = (sent[mine, part] if d == 0 else landed[d + half, part]).astype(jnp.float32)
            for h in range(heads):
                merged[c + h] += column(share, c + h) * values[h * group : (h + 1) * group]
    for branch in range(2):
        board[me, branch * tile : (branch + 1) * tile] = jnp.concatenate(
            merged[branch * heads : (branch + 1) * heads], axis=0
        ).astype(jnp.bfloat16)
    board[me, 2 * tile :] = split_logs(jnp.where(lane < 2 * heads, top + jnp.log(total), 0.0))

    def broadcast(owner, offset, number):
        return remote(board.at[owner], board.at[owner], b_send.at[number], b_recv.at[owner], at(offset))

    steps = []
    for distance in range(STRIDE, n // 2, STRIDE):
        steps += [distance, -distance]
    steps.append(n // 2)
    second_copies = []

    def start(owner, offset):
        copy = broadcast(owner, offset, len(second_copies))
        copy.start()
        second_copies.append(copy)

    for offset in reversed(steps):
        start(me, offset)
    for near in NEAR:
        start(me, near)
    for offset in steps:
        owner = at(-offset)
        broadcast(owner, offset, 0).wait_recv()
        for near in NEAR:
            start(owner, near)
    for offset in [0] + steps:
        for near in NEAR:
            broadcast(at(-offset - near), near, 0).wait_recv()

    for b in range(rows):
        logs = [join_logs(board[s * window + b, 2 * tile :]) for s in range(sources)]
        top = functools.reduce(jnp.maximum, logs)
        shares = [jnp.exp(x - top) for x in logs]
        factor = gates[b] / functools.reduce(jnp.add, shares)
        mixed = [jnp.zeros((group, width), jnp.float32) for _ in range(heads)]
        for s, share in enumerate(shares):
            share = share * factor
            for branch in range(2):
                values = board[s * window + b, branch * tile : (branch + 1) * tile].astype(jnp.float32)
                for h in range(heads):
                    mixed[h] += column(share, branch * heads + h) * values[h * group : (h + 1) * group]
        out_ref[b] = jnp.concatenate(mixed, axis=0).astype(jnp.bfloat16)

    for copy in first_copies + second_copies:
        copy.wait_send()


def on_device(n, queries, key_cache, value_cache, gate_logits, lengths, chosen, counts):
    rows, heads, context, width = key_cache.shape
    group = queries.shape[1] // heads
    window = rows
    lines = 2 * heads * group + group
    relays = len(range(STRIDE, n // 2, STRIDE)) * 2 + 1
    vmem = pl.BlockSpec(memory_space=pltpu.VMEM)
    smem = pl.BlockSpec(memory_space=pltpu.SMEM)
    anywhere = pl.BlockSpec(memory_space=pl.ANY)
    return pl.pallas_call(
        functools.partial(kernel, n),
        name="decode",
        out_shape=jax.ShapeDtypeStruct(queries.shape, jnp.bfloat16),
        in_specs=[vmem, anywhere, anywhere, vmem, smem, vmem, smem],
        out_specs=vmem,
        scratch_shapes=[
            pltpu.VMEM(key_cache.shape, jnp.bfloat16),
            pltpu.VMEM(value_cache.shape, jnp.bfloat16),
            pltpu.VMEM((rows, lines, width), jnp.bfloat16),
            pltpu.VMEM((window, lines, width), jnp.bfloat16),
            pltpu.VMEM((n, lines, width), jnp.bfloat16),
            pltpu.VMEM((width, width), jnp.float32),
            pltpu.VMEM((rows, group, width), jnp.float32),
            pltpu.SemaphoreType.DMA((rows // CHUNK,)),
            pltpu.SemaphoreType.DMA((rows // CHUNK,)),
            pltpu.SemaphoreType.DMA((window,)),
            pltpu.SemaphoreType.DMA((window,)),
            pltpu.SemaphoreType.DMA((relays + len(NEAR) * (relays + 1),)),
            pltpu.SemaphoreType.DMA((n,)),
        ],
        compiler_params=pltpu.CompilerParams(collective_id=0, has_side_effects=True),
    )(queries, key_cache, value_cache, gate_logits, lengths, chosen, counts.T)


def solution(mesh):
    return jax.shard_map(
        functools.partial(on_device, mesh.shape["seq"]),
        mesh=mesh,
        in_specs=(
            P(("grp", "batch"), "head", None),
            P(("grp", "batch"), "head", "seq", None),
            P(("grp", "batch"), "head", "seq", None),
            P(None, ("grp", "batch"), "head"),
            P(("grp", "batch")),
            P(("grp", "batch"), "head", None),
            P(("grp", "batch"), "head"),
        ),
        out_specs=P(("grp", "batch"), "head", None),
        check_vma=False,
    )
```

```python
import functools
import math

import jax
import jax.numpy as jnp
from jax import lax
from jax.experimental import pallas as pl
from jax.experimental.pallas import tpu as pltpu
from jax.sharding import PartitionSpec as P

BLOCK = 128
STRIDE = 4
NEAR = (-1, 1, 2)
CHUNK = 4
LOADS = 2
PIECE = 32
NEG = -1e30
MESH = pl.DeviceIdType.MESH


def iota(shape, dim):
    return lax.broadcasted_iota(jnp.int32, shape, dim)


def split_logs(logs):
    lane = iota(logs.shape, 1)
    spread = jnp.where(
        lane < PIECE,
        logs,
        jnp.where(lane < 2 * PIECE, pltpu.roll(logs, PIECE, 1), pltpu.roll(logs, 2 * PIECE, 1)),
    )
    high = spread.astype(jnp.bfloat16).astype(jnp.float32)
    rest = spread - high
    middle = rest.astype(jnp.bfloat16).astype(jnp.float32)
    low = rest - middle
    return jnp.where(lane < PIECE, high, jnp.where(lane < 2 * PIECE, middle, low)).astype(jnp.bfloat16)


def join_logs(pieces):
    pieces = pieces.astype(jnp.float32)
    width = pieces.shape[1]
    return (pieces + pltpu.roll(pieces, width - PIECE, 1)) + pltpu.roll(pieces, width - 2 * PIECE, 1)


def column(tile, lane):
    return jnp.broadcast_to(tile[:, lane : lane + 1], tile.shape)


def kernel(
    n,
    q_ref,
    k_hbm,
    v_hbm,
    gate_ref,
    length_ref,
    chosen_ref,
    count_ref,
    out_ref,
    k_buf,
    v_buf,
    sent,
    landed,
    board,
    gate_pad,
    gates,
    scores,
    k_sem,
    v_sem,
    a_send,
    a_recv,
    b_send,
    hop_recv,
    near_recv,
):
    me = lax.axis_index("seq")
    sign = 1 - 2 * lax.axis_index("batch")
    rows, heads, context, width = k_buf.shape
    group = q_ref.shape[1] // heads
    local = context // BLOCK
    window = rows
    half = window // 2
    sources = n // window
    tile = heads * group
    scale = 1.0 / math.sqrt(width)

    def at(offset):
        return lax.rem(me + sign * offset + 2 * n, n)

    def remote(src, dst, send, recv, target):
        return pltpu.make_async_remote_copy(
            src_ref=src,
            dst_ref=dst,
            send_sem=send,
            recv_sem=recv,
            device_id={"seq": target},
            device_id_type=MESH,
        )

    barrier = pltpu.get_barrier_semaphore()
    for distance in range(half, 0, -1):
        for offset in (-distance, distance):
            pl.semaphore_signal(barrier, inc=1, device_id={"seq": at(offset)}, device_id_type=MESH)

    def load(which, c):
        part = pl.ds(c * (rows // LOADS), rows // LOADS)
        source, target, sem = (v_hbm, v_buf, v_sem) if which else (k_hbm, k_buf, k_sem)
        return pltpu.make_async_copy(source.at[part], target.at[part], sem.at[c])

    for which in range(2):
        for c in range(LOADS):
            load(which, c).start()

    gate_pad[...] = jnp.zeros_like(gate_pad)
    for branch in range(2):
        logits = gate_ref[branch]
        gate_pad[branch * rows : (branch + 1) * rows, : heads * group] = 1.0 / (1.0 + jnp.exp(-logits))
    turned = gate_pad[...].T
    lane = iota((group, width), 1)
    for b in range(rows):
        packed = jnp.zeros((group, width), jnp.float32)
        for branch in range(2):
            for h in range(heads):
                c = branch * heads + h
                here = turned[h * group : (h + 1) * group]
                moved = pltpu.roll(here, (c - (1 - branch) * rows - b) % width, 1)
                packed = jnp.where(lane == c, moved, packed)
        gates[b] = packed

    slot = iota((1, chosen_ref.shape[2]), 1)
    first = me * local

    def one_pair(b, h, live, root):
        parts = [scores[b, h, :, j * BLOCK : (j + 1) * BLOCK] for j in range(local)]
        chosen = chosen_ref[b, h : h + 1, :]
        listed = slot < count_ref[h, b]
        masks = []
        for j in range(local):
            hit = jnp.where((chosen == first + j) & listed, 1.0, 0.0)
            picked = jnp.max(hit, axis=1, keepdims=True)
            masks.append(live[j] & (jnp.broadcast_to(picked, (group, BLOCK)) > 0.5))
        kept = [jnp.where(m, s, NEG) for m, s in zip(masks, parts)]
        top = jnp.max(functools.reduce(jnp.maximum, kept), axis=1, keepdims=True)
        weights = [jnp.where(m, jnp.exp(s - top), 0.0) for m, s in zip(masks, kept)]
        total = jnp.sum(sum(weights), axis=1, keepdims=True)
        pooled = [
            jnp.where(
                live[j][:, :1],
                jnp.sum(jnp.where(live[j], parts[j], 0.0), axis=1, keepdims=True) * root[j],
                NEG,
            )
            for j in range(local)
        ]
        pool_top = functools.reduce(jnp.maximum, pooled)
        pool_weights = [jnp.where(live[j][:, :1], jnp.exp(pooled[j] - pool_top), 0.0) for j in range(local)]
        pool_total = sum(pool_weights)
        spread = [jnp.where(live[j], pool_weights[j] * root[j], 0.0) for j in range(local)]
        left = jnp.concatenate(
            [jnp.concatenate(weights, axis=1), jnp.concatenate(spread, axis=1)], axis=0
        ).astype(jnp.bfloat16)
        summed = jnp.dot(left, v_buf[b, h], preferred_element_type=jnp.float32)
        result = []
        for top_of, total_of, value in (
            (top, total, summed[:group]),
            (pool_top, pool_total, summed[group:]),
        ):
            some = total_of > 0.0
            safe = jnp.where(some, total_of, 1.0)
            result.append((value / safe, jnp.where(some, top_of + jnp.log(safe), NEG)))
        return result

    def one_row(b):
        length = length_ref[b]
        live, root = [], []
        for j in range(local):
            start = (first + j) * BLOCK
            live.append(start + iota((group, BLOCK), 1) < length)
            filled = jnp.clip(length - start, 1, BLOCK).astype(jnp.float32)
            root.append(1.0 / jnp.sqrt(jnp.full((group, 1), filled, jnp.float32)))
        pairs = [one_pair(b, h, live, root) for h in range(heads)]
        logs = jnp.zeros((group, width), jnp.float32)
        for branch in range(2):
            values = jnp.concatenate([pairs[h][branch][0] for h in range(heads)], axis=0)
            sent[b, branch * tile : (branch + 1) * tile] = values.astype(jnp.bfloat16)
            for h in range(heads):
                logs = jnp.where(lane == branch * heads + h, pairs[h][branch][1], logs)
        sent[b, 2 * tile :] = split_logs(logs)

    def score_chunk(c, carry):
        for i in range(CHUNK):
            b = c * CHUNK + i
            for h in range(heads):
                product = lax.dot_general(
                    q_ref[b], k_buf[b, h], (((1,), (1,)), ((), ())), preferred_element_type=jnp.float32
                )
                scores[b, h] = product[h * group : (h + 1) * group] * scale
        return carry

    def value_chunk(c, carry):
        for i in range(CHUNK):
            one_row(c * CHUNK + i)
        return carry

    per_load = rows // LOADS // CHUNK
    for which, chunk in ((0, score_chunk), (1, value_chunk)):
        for c in range(LOADS):
            load(which, c).wait()
            lax.fori_loop(c * per_load, (c + 1) * per_load, chunk, 0)

    pl.semaphore_wait(barrier, 2 * half)
    offsets = sorted((d for d in range(-half, half) if d != 0), key=lambda d: -abs(d))
    for i, offset in enumerate(offsets):
        target = at(offset)
        remote(sent.at[lax.rem(target, window)], landed.at[i], a_send, a_recv, target).start()
    arrivals = pl.ds(0, len(offsets))
    first_copies = remote(sent.at[arrivals], landed.at[arrivals], a_send, a_recv, at(1))
    first_copies.wait_recv()

    mine = lax.rem(me, window)
    logs = [
        join_logs(sent[mine, 2 * tile :] if i < 0 else landed[i, 2 * tile :])
        for i in range(-1, len(offsets))
    ]
    top = functools.reduce(jnp.maximum, logs)
    shares = [jnp.exp(x - top) for x in logs]
    total = functools.reduce(jnp.add, shares)
    merged = [jnp.zeros((group, width), jnp.float32) for _ in range(2 * heads)]
    inverse = 1.0 / total
    for share, i in zip(shares, range(-1, len(offsets))):
        share = share * inverse
        for c in range(0, 2 * heads, heads):
            part = pl.ds(c * group, tile)
            values = (sent[mine, part] if i < 0 else landed[i, part]).astype(jnp.float32)
            for h in range(heads):
                merged[c + h] += column(share, c + h) * values[h * group : (h + 1) * group]
    for branch in range(2):
        board[me, branch * tile : (branch + 1) * tile] = jnp.concatenate(
            merged[branch * heads : (branch + 1) * heads], axis=0
        ).astype(jnp.bfloat16)
    board[me, 2 * tile :] = split_logs(jnp.where(lane < 2 * heads, top + jnp.log(total), 0.0))

    steps = []
    for distance in range(STRIDE, n // 2, STRIDE):
        steps += [distance, -distance]
    steps.append(n // 2)

    def hop(number, owner):
        return remote(board.at[owner], board.at[owner], b_send, hop_recv.at[number], at(steps[number]))

    def pass_on(owner):
        for near in NEAR:
            remote(board.at[owner], board.at[owner], b_send, near_recv, at(near)).start()

    for number in reversed(range(len(steps))):
        hop(number, me).start()
    pass_on(me)
    for number, offset in enumerate(steps):
        owner = at(-offset)
        hop(number, owner).wait_recv()
        pass_on(owner)
    passed = pl.ds(0, len(NEAR) * (len(steps) + 1))
    remote(board.at[passed], board.at[passed], b_send, near_recv, at(1)).wait_recv()

    for b in range(rows):
        logs = [join_logs(board[s * window + b, 2 * tile :]) for s in range(sources)]
        top = functools.reduce(jnp.maximum, logs)
        shares = [jnp.exp(x - top) for x in logs]
        factor = gates[b] / functools.reduce(jnp.add, shares)
        mixed = [jnp.zeros((group, width), jnp.float32) for _ in range(heads)]
        for s, share in enumerate(shares):
            share = share * factor
            for branch in range(2):
                values = board[s * window + b, branch * tile : (branch + 1) * tile].astype(jnp.float32)
                for h in range(heads):
                    mixed[h] += column(share, branch * heads + h) * values[h * group : (h + 1) * group]
        out_ref[b] = jnp.concatenate(mixed, axis=0).astype(jnp.bfloat16)

    first_copies.wait_send()
    everything = pl.ds(0, n - 1)
    remote(board.at[everything], board.at[everything], b_send, near_recv, at(1)).wait_send()


def on_device(n, queries, key_cache, value_cache, gate_logits, lengths, chosen, counts):
    rows, heads, context, width = key_cache.shape
    group = queries.shape[1] // heads
    window = rows
    lines = 2 * heads * group + group
    relays = len(range(STRIDE, n // 2, STRIDE)) * 2 + 1
    vmem = pl.BlockSpec(memory_space=pltpu.VMEM)
    smem = pl.BlockSpec(memory_space=pltpu.SMEM)
    anywhere = pl.BlockSpec(memory_space=pl.ANY)
    return pl.pallas_call(
        functools.partial(kernel, n),
        name="decode",
        out_shape=jax.ShapeDtypeStruct(queries.shape, jnp.bfloat16),
        in_specs=[vmem, anywhere, anywhere, vmem, smem, vmem, smem],
        out_specs=vmem,
        scratch_shapes=[
            pltpu.VMEM(key_cache.shape, jnp.bfloat16),
            pltpu.VMEM(value_cache.shape, jnp.bfloat16),
            pltpu.VMEM((rows, lines, width), jnp.bfloat16),
            pltpu.VMEM((window, lines, width), jnp.bfloat16),
            pltpu.VMEM((n, lines, width), jnp.bfloat16),
            pltpu.VMEM((width, width), jnp.float32),
            pltpu.VMEM((rows, group, width), jnp.float32),
            pltpu.VMEM((rows, heads, group, context), jnp.float32),
            pltpu.SemaphoreType.DMA((LOADS,)),
            pltpu.SemaphoreType.DMA((LOADS,)),
            pltpu.SemaphoreType.DMA,
            pltpu.SemaphoreType.DMA,
            pltpu.SemaphoreType.DMA,
            pltpu.SemaphoreType.DMA((relays,)),
            pltpu.SemaphoreType.DMA,
        ],
        compiler_params=pltpu.CompilerParams(collective_id=0, has_side_effects=True),
    )(queries, key_cache, value_cache, gate_logits, lengths, chosen, counts.T)


def solution(mesh):
    return jax.shard_map(
        functools.partial(on_device, mesh.shape["seq"]),
        mesh=mesh,
        in_specs=(
            P(("grp", "batch"), "head", None),
            P(("grp", "batch"), "head", "seq", None),
            P(("grp", "batch"), "head", "seq", None),
            P(None, ("grp", "batch"), "head"),
            P(("grp", "batch")),
            P(("grp", "batch"), "head", None),
            P(("grp", "batch"), "head"),
        ),
        out_specs=P(("grp", "batch"), "head", None),
        check_vma=False,
    )
```

```python
import functools
import math

import jax
import jax.numpy as jnp
from jax import lax
from jax.experimental import pallas as pl
from jax.experimental.pallas import tpu as pltpu
from jax.sharding import PartitionSpec as P

BLOCK = 128
WINDOW = 8
ROOT = 1
STRIDE = 4
CHUNK = 4
LOADS = 2
PIECE = 32
NEG = -1e30
MESH = pl.DeviceIdType.MESH


def iota(shape, dim):
    return lax.broadcasted_iota(jnp.int32, shape, dim)


def split_logs(logs):
    lane = iota(logs.shape, 1)
    spread = jnp.where(
        lane < PIECE,
        logs,
        jnp.where(lane < 2 * PIECE, pltpu.roll(logs, PIECE, 1), pltpu.roll(logs, 2 * PIECE, 1)),
    )
    high = spread.astype(jnp.bfloat16).astype(jnp.float32)
    rest = spread - high
    middle = rest.astype(jnp.bfloat16).astype(jnp.float32)
    low = rest - middle
    return jnp.where(lane < PIECE, high, jnp.where(lane < 2 * PIECE, middle, low)).astype(jnp.bfloat16)


def join_logs(pieces):
    pieces = pieces.astype(jnp.float32)
    width = pieces.shape[1]
    return (pieces + pltpu.roll(pieces, width - PIECE, 1)) + pltpu.roll(pieces, width - 2 * PIECE, 1)


def column(tile, lane):
    return jnp.broadcast_to(tile[:, lane : lane + 1], tile.shape)


def kernel(
    n,
    q_ref,
    k_hbm,
    v_hbm,
    gate_ref,
    length_ref,
    chosen_ref,
    count_ref,
    out_ref,
    k_buf,
    v_buf,
    sent,
    landed,
    board,
    gate_pad,
    gates,
    scores,
    k_sem,
    v_sem,
    a_send,
    a_recv,
    b_send,
    b_recv,
    c_send,
    c_recv,
):
    me = lax.axis_index("seq")
    sign = 1 - 2 * lax.axis_index("batch")
    rows, heads, context, width = k_buf.shape
    group = q_ref.shape[1] // heads
    local = context // BLOCK
    half = WINDOW // 2
    sources = n // WINDOW
    per = rows // WINDOW
    tile = heads * group
    scale = 1.0 / math.sqrt(width)

    def at(offset):
        return lax.rem(me + sign * offset + n, n)

    def remote(src, dst, send, recv, target):
        return pltpu.make_async_remote_copy(
            src_ref=src,
            dst_ref=dst,
            send_sem=send,
            recv_sem=recv,
            device_id={"seq": target},
            device_id_type=MESH,
        )

    root = ROOT
    away = lax.rem(sign * (root - me) + n, n)
    outside = (away > half) & (away < n - half)
    barrier = pltpu.get_barrier_semaphore()
    for distance in range(half, 0, -1):
        for offset in (-distance, distance):
            pl.semaphore_signal(barrier, inc=1, device_id={"seq": at(offset)}, device_id_type=MESH)

    @pl.when(me == root)
    def _():
        for offset in range(half + 1, n - half):
            pl.semaphore_signal(barrier, inc=1, device_id={"seq": at(offset)}, device_id_type=MESH)

    def load(which, c):
        part = pl.ds(c * (rows // LOADS), rows // LOADS)
        source, target, sem = (v_hbm, v_buf, v_sem) if which else (k_hbm, k_buf, k_sem)
        return pltpu.make_async_copy(source.at[part], target.at[part], sem.at[c])

    for which in range(2):
        for c in range(LOADS):
            load(which, c).start()

    gate_pad[...] = jnp.zeros_like(gate_pad)
    for branch in range(2):
        logits = gate_ref[branch]
        gate_pad[branch * rows : (branch + 1) * rows, : heads * group] = 1.0 / (1.0 + jnp.exp(-logits))
    turned = gate_pad[...].T
    lane = iota((group, width), 1)
    for block in range(WINDOW):
        packed = jnp.zeros((group, width), jnp.float32)
        for k in range(per):
            for branch in range(2):
                for h in range(heads):
                    c = (2 * k + branch) * heads + h
                    here = turned[h * group : (h + 1) * group]
                    moved = pltpu.roll(here, (c - (1 - branch) * rows - block * per - k) % width, 1)
                    packed = jnp.where(lane == c, moved, packed)
        gates[block] = packed

    slot = iota((1, chosen_ref.shape[2]), 1)
    first = me * local

    def one_pair(b, h, live, root):
        parts = [scores[b, h, :, j * BLOCK : (j + 1) * BLOCK] for j in range(local)]
        chosen = chosen_ref[b, h : h + 1, :]
        listed = slot < count_ref[h, b]
        masks = []
        for j in range(local):
            hit = jnp.where((chosen == first + j) & listed, 1.0, 0.0)
            picked = jnp.max(hit, axis=1, keepdims=True)
            masks.append(live[j] & (jnp.broadcast_to(picked, (group, BLOCK)) > 0.5))
        kept = [jnp.where(m, s, NEG) for m, s in zip(masks, parts)]
        top = jnp.max(functools.reduce(jnp.maximum, kept), axis=1, keepdims=True)
        weights = [jnp.where(m, jnp.exp(s - top), 0.0) for m, s in zip(masks, kept)]
        total = jnp.sum(sum(weights), axis=1, keepdims=True)
        pooled = [
            jnp.where(
                live[j][:, :1],
                jnp.sum(jnp.where(live[j], parts[j], 0.0), axis=1, keepdims=True) * root[j],
                NEG,
            )
            for j in range(local)
        ]
        pool_top = functools.reduce(jnp.maximum, pooled)
        pool_weights = [jnp.where(live[j][:, :1], jnp.exp(pooled[j] - pool_top), 0.0) for j in range(local)]
        pool_total = sum(pool_weights)
        spread = [jnp.where(live[j], pool_weights[j] * root[j], 0.0) for j in range(local)]
        left = jnp.concatenate(
            [jnp.concatenate(weights, axis=1), jnp.concatenate(spread, axis=1)], axis=0
        ).astype(jnp.bfloat16)
        summed = jnp.dot(left, v_buf[b, h], preferred_element_type=jnp.float32)
        result = []
        for top_of, total_of, value in (
            (top, total, summed[:group]),
            (pool_top, pool_total, summed[group:]),
        ):
            some = total_of > 0.0
            safe = jnp.where(some, total_of, 1.0)
            result.append((value / safe, jnp.where(some, top_of + jnp.log(safe), NEG)))
        return result

    def one_row(b, block, k, logs):
        length = length_ref[b]
        live, root = [], []
        for j in range(local):
            start = (first + j) * BLOCK
            live.append(start + iota((group, BLOCK), 1) < length)
            filled = jnp.clip(length - start, 1, BLOCK).astype(jnp.float32)
            root.append(1.0 / jnp.sqrt(jnp.full((group, 1), filled, jnp.float32)))
        pairs = [one_pair(b, h, live, root) for h in range(heads)]
        for branch in range(2):
            values = jnp.concatenate([pairs[h][branch][0] for h in range(heads)], axis=0)
            sent[block, pl.ds((2 * k + branch) * tile, tile)] = values.astype(jnp.bfloat16)
            for h in range(heads):
                logs = jnp.where(lane == (2 * k + branch) * heads + h, pairs[h][branch][1], logs)
        return logs

    def score_chunk(c, carry):
        for i in range(CHUNK):
            b = c * CHUNK + i
            for h in range(heads):
                product = lax.dot_general(
                    q_ref[b], k_buf[b, h], (((1,), (1,)), ((), ())), preferred_element_type=jnp.float32
                )
                scores[b, h] = product[h * group : (h + 1) * group] * scale
        return carry

    def value_chunk(c, carry):
        for i in range(CHUNK // per):
            block = c * (CHUNK // per) + i
            logs = jnp.zeros((group, width), jnp.float32)
            for k in range(per):
                logs = one_row(block * per + k, block, k, logs)
            sent[block, 2 * per * tile :] = split_logs(logs)
        return carry

    per_load = rows // LOADS // CHUNK
    for which, chunk in ((0, score_chunk), (1, value_chunk)):
        for c in range(LOADS):
            load(which, c).wait()
            lax.fori_loop(c * per_load, (c + 1) * per_load, chunk, 0)

    pl.semaphore_wait(barrier, 2 * half + outside.astype(jnp.int32))
    offsets = sorted((d for d in range(-half, half) if d != 0), key=lambda d: -abs(d))
    for i, offset in enumerate(offsets):
        target = at(offset)
        remote(sent.at[lax.rem(target, WINDOW)], landed.at[i], a_send, a_recv, target).start()
    arrivals = pl.ds(0, len(offsets))
    first_copies = remote(sent.at[arrivals], landed.at[arrivals], a_send, a_recv, at(1))
    first_copies.wait_recv()

    mine = lax.rem(me, WINDOW)
    logs = [join_logs(sent[mine, 2 * per * tile :] if i < 0 else landed[i, 2 * per * tile :]) for i in range(-1, len(offsets))]
    top = functools.reduce(jnp.maximum, logs)
    shares = [jnp.exp(x - top) for x in logs]
    total = functools.reduce(jnp.add, shares)
    inverse = 1.0 / total
    merged = [jnp.zeros((group, width), jnp.float32) for _ in range(2 * per * heads)]
    for share, i in zip(shares, range(-1, len(offsets))):
        share = share * inverse
        for c in range(0, len(merged), heads):
            part = pl.ds(c * group, tile)
            values = (sent[mine, part] if i < 0 else landed[i, part]).astype(jnp.float32)
            for h in range(heads):
                merged[c + h] += column(share, c + h) * values[h * group : (h + 1) * group]
    for c in range(0, len(merged), heads):
        board[me, c * group : c * group + tile] = jnp.concatenate(merged[c : c + heads], axis=0).astype(jnp.bfloat16)
    board[me, 2 * per * tile :] = split_logs(jnp.where(lane < len(merged), top + jnp.log(total), 0.0))

    relays = n // STRIDE
    up = relays // 2 + 1
    split = relays // 4

    def spread(k):
        steps = [STRIDE] if k < up else []
        steps += [-(split + 1) * STRIDE] if k == split else []
        steps += [-STRIDE] if up + 1 < k else []
        copies = []
        for i, step in enumerate([-1] + steps + [1, 2]):
            target = (ROOT + k * STRIDE + step) % n
            copies.append(remote(out_ref, out_ref, c_send.at[i], c_recv, target))
            copies[-1].start()
        for copy in copies:
            copy.wait_send()

    @pl.when(me != root)
    def _():
        block = remote(board.at[me], board.at[me], b_send, b_recv, root)
        block.start()
        block.wait_send()
        remote(out_ref, out_ref, c_send.at[0], c_recv, root).wait_recv()
        for k in range(1, relays):

            @pl.when(me == (ROOT + k * STRIDE) % n)
            def _(k=k):
                spread(k)

    @pl.when(me == root)
    def _():
        others = pl.ds(0, n - 1)
        remote(board.at[others], board.at[others], b_send, b_recv, at(1)).wait_recv()
        for block in range(WINDOW):
            logs = [join_logs(board[s * WINDOW + block, 2 * per * tile :]) for s in range(sources)]
            top = functools.reduce(jnp.maximum, logs)
            shares = [jnp.exp(x - top) for x in logs]
            inverse = 1.0 / functools.reduce(jnp.add, shares)
            factor = gates[block] * inverse
            shares = [x * factor for x in shares]
            for k in range(per):
                mixed = [jnp.zeros((group, width), jnp.float32) for _ in range(heads)]
                for s, share in enumerate(shares):
                    for branch in range(2):
                        c = (2 * k + branch) * heads
                        values = board[s * WINDOW + block, c * group : c * group + tile].astype(jnp.float32)
                        for h in range(heads):
                            mixed[h] += column(share, c + h) * values[h * group : (h + 1) * group]
                out_ref[block * per + k] = jnp.concatenate(mixed, axis=0).astype(jnp.bfloat16)

        spread(0)

    first_copies.wait_send()


def on_device(n, queries, key_cache, value_cache, gate_logits, lengths, chosen, counts):
    rows, heads, context, width = key_cache.shape
    group = queries.shape[1] // heads
    lines = rows // WINDOW * 2 * heads * group + group
    vmem = pl.BlockSpec(memory_space=pltpu.VMEM)
    smem = pl.BlockSpec(memory_space=pltpu.SMEM)
    anywhere = pl.BlockSpec(memory_space=pl.ANY)
    return pl.pallas_call(
        functools.partial(kernel, n),
        name="decode",
        out_shape=pltpu.VMEM(queries.shape, jnp.bfloat16),
        in_specs=[vmem, anywhere, anywhere, vmem, smem, vmem, smem],
        out_specs=vmem,
        scratch_shapes=[
            pltpu.VMEM(key_cache.shape, jnp.bfloat16),
            pltpu.VMEM(value_cache.shape, jnp.bfloat16),
            pltpu.VMEM((WINDOW, lines, width), jnp.bfloat16),
            pltpu.VMEM((WINDOW - 1, lines, width), jnp.bfloat16),
            pltpu.VMEM((n, lines, width), jnp.bfloat16),
            pltpu.VMEM((width, width), jnp.float32),
            pltpu.VMEM((WINDOW, group, width), jnp.float32),
            pltpu.VMEM((rows, heads, group, context), jnp.float32),
            pltpu.SemaphoreType.DMA((LOADS,)),
            pltpu.SemaphoreType.DMA((LOADS,)),
            pltpu.SemaphoreType.DMA,
            pltpu.SemaphoreType.DMA,
            pltpu.SemaphoreType.DMA,
            pltpu.SemaphoreType.DMA,
            pltpu.SemaphoreType.DMA((5,)),
            pltpu.SemaphoreType.DMA,
        ],
        compiler_params=pltpu.CompilerParams(collective_id=0, has_side_effects=True),
    )(queries, key_cache, value_cache, gate_logits, lengths, chosen, counts.T)


def solution(mesh):
    return jax.shard_map(
        functools.partial(on_device, mesh.shape["seq"]),
        mesh=mesh,
        in_specs=(
            P(("grp", "batch"), "head", None),
            P(("grp", "batch"), "head", "seq", None),
            P(("grp", "batch"), "head", "seq", None),
            P(None, ("grp", "batch"), "head"),
            P(("grp", "batch")),
            P(("grp", "batch"), "head", None),
            P(("grp", "batch"), "head"),
        ),
        out_specs=P(("grp", "batch"), "head", None),
        check_vma=False,
    )
```

```python
import functools
import math

import jax
import jax.numpy as jnp
from jax import lax
from jax.experimental import pallas as pl
from jax.experimental.pallas import tpu as pltpu
from jax.sharding import PartitionSpec as P

BLOCK = 128
WINDOW = 8
ROOT = 1
STRIDE = 4
PARTS = 4
CHUNK = 4
LOADS = 2
PIECE = 32
NEG = -1e30
MESH = pl.DeviceIdType.MESH


def iota(shape, dim):
    return lax.broadcasted_iota(jnp.int32, shape, dim)


def split_logs(logs):
    lane = iota(logs.shape, 1)
    spread = jnp.where(
        lane < PIECE,
        logs,
        jnp.where(lane < 2 * PIECE, pltpu.roll(logs, PIECE, 1), pltpu.roll(logs, 2 * PIECE, 1)),
    )
    high = spread.astype(jnp.bfloat16).astype(jnp.float32)
    rest = spread - high
    middle = rest.astype(jnp.bfloat16).astype(jnp.float32)
    low = rest - middle
    return jnp.where(lane < PIECE, high, jnp.where(lane < 2 * PIECE, middle, low)).astype(jnp.bfloat16)


def join_logs(pieces):
    pieces = pieces.astype(jnp.float32)
    width = pieces.shape[1]
    return (pieces + pltpu.roll(pieces, width - PIECE, 1)) + pltpu.roll(pieces, width - 2 * PIECE, 1)


def column(tile, lane):
    return jnp.broadcast_to(tile[:, lane : lane + 1], tile.shape)


def kernel(
    n,
    q_hbm,
    k_hbm,
    v_hbm,
    gate_hbm,
    length_hbm,
    chosen_hbm,
    count_hbm,
    out_ref,
    q_ref,
    gate_ref,
    length_ref,
    chosen_ref,
    count_ref,
    k_buf,
    v_buf,
    sent,
    landed,
    board,
    gate_pad,
    gates,
    scores,
    in_sem,
    k_sem,
    v_sem,
    a_send,
    a_recv,
    b_send,
    b_recv,
    c_send,
    c_recv,
):
    me = lax.axis_index("seq")
    rows, heads, context, width = k_buf.shape
    group = q_ref.shape[1] // heads
    local = context // BLOCK
    half = WINDOW // 2
    sources = n // WINDOW
    per = rows // WINDOW
    tile = heads * group
    scale = 1.0 / math.sqrt(width)

    def at(offset):
        return lax.rem(me + offset + n, n)

    def remote(src, dst, send, recv, target):
        return pltpu.make_async_remote_copy(
            src_ref=src,
            dst_ref=dst,
            send_sem=send,
            recv_sem=recv,
            device_id={"seq": target},
            device_id_type=MESH,
        )

    def load(which, c):
        part = pl.ds(c * (rows // LOADS), rows // LOADS)
        source, target, sem = (v_hbm, v_buf, v_sem) if which else (k_hbm, k_buf, k_sem)
        return pltpu.make_async_copy(source.at[part], target.at[part], sem.at[c])

    small = [
        pltpu.make_async_copy(source, target, in_sem.at[i])
        for i, (source, target) in enumerate(
            (
                (q_hbm, q_ref),
                (length_hbm, length_ref),
                (chosen_hbm, chosen_ref),
                (count_hbm, count_ref),
                (gate_hbm, gate_ref),
            )
        )
    ]
    small[0].start()
    for c in range(LOADS):
        load(0, c).start()
    for copy in small[1:]:
        copy.start()
    for c in range(LOADS):
        load(1, c).start()

    root = ROOT
    away = lax.rem(root - me + n, n)
    outside = (away > half) & (away < n - half)
    barrier = pltpu.get_barrier_semaphore()
    for distance in range(half, 0, -1):
        for offset in (-distance, distance):
            pl.semaphore_signal(barrier, inc=1, device_id={"seq": at(offset)}, device_id_type=MESH)

    @pl.when(me == root)
    def _():
        for offset in range(half + 1, n - half):
            pl.semaphore_signal(barrier, inc=1, device_id={"seq": at(offset)}, device_id_type=MESH)

    lane = iota((group, width), 1)
    slot = iota((1, chosen_ref.shape[2]), 1)
    first = me * local

    def one_pair(b, h, live, root):
        parts = [scores[b, h, :, j * BLOCK : (j + 1) * BLOCK] for j in range(local)]
        chosen = chosen_ref[b, h : h + 1, :]
        listed = slot < count_ref[h, b]
        masks = []
        for j in range(local):
            hit = jnp.where((chosen == first + j) & listed, 1.0, 0.0)
            picked = jnp.max(hit, axis=1, keepdims=True)
            masks.append(live[j] & (jnp.broadcast_to(picked, (group, BLOCK)) > 0.5))
        kept = [jnp.where(m, s, NEG) for m, s in zip(masks, parts)]
        top = jnp.max(functools.reduce(jnp.maximum, kept), axis=1, keepdims=True)
        weights = [jnp.where(m, jnp.exp(s - top), 0.0) for m, s in zip(masks, kept)]
        total = jnp.sum(sum(weights), axis=1, keepdims=True)
        pooled = [
            jnp.where(
                live[j][:, :1],
                jnp.sum(jnp.where(live[j], parts[j], 0.0), axis=1, keepdims=True) * root[j],
                NEG,
            )
            for j in range(local)
        ]
        pool_top = functools.reduce(jnp.maximum, pooled)
        pool_weights = [jnp.where(live[j][:, :1], jnp.exp(pooled[j] - pool_top), 0.0) for j in range(local)]
        pool_total = sum(pool_weights)
        spread = [jnp.where(live[j], pool_weights[j] * root[j], 0.0) for j in range(local)]
        left = jnp.concatenate(
            [jnp.concatenate(weights, axis=1), jnp.concatenate(spread, axis=1)], axis=0
        ).astype(jnp.bfloat16)
        summed = jnp.dot(left, v_buf[b, h], preferred_element_type=jnp.float32)
        result = []
        for top_of, total_of, value in (
            (top, total, summed[:group]),
            (pool_top, pool_total, summed[group:]),
        ):
            some = total_of > 0.0
            safe = jnp.where(some, total_of, 1.0)
            result.append((value / safe, jnp.where(some, top_of + jnp.log(safe), NEG)))
        return result

    def one_row(b, block, k, logs):
        length = length_ref[b]
        live, root = [], []
        for j in range(local):
            start = (first + j) * BLOCK
            live.append(start + iota((group, BLOCK), 1) < length)
            filled = jnp.clip(length - start, 1, BLOCK).astype(jnp.float32)
            root.append(1.0 / jnp.sqrt(jnp.full((group, 1), filled, jnp.float32)))
        pairs = [one_pair(b, h, live, root) for h in range(heads)]
        for branch in range(2):
            values = jnp.concatenate([pairs[h][branch][0] for h in range(heads)], axis=0)
            sent[block, pl.ds((2 * k + branch) * tile, tile)] = values.astype(jnp.bfloat16)
            for h in range(heads):
                logs = jnp.where(lane == (2 * k + branch) * heads + h, pairs[h][branch][1], logs)
        return logs

    def score_chunk(c, carry):
        for i in range(CHUNK):
            b = c * CHUNK + i
            for h in range(heads):
                product = lax.dot_general(
                    q_ref[b], k_buf[b, h], (((1,), (1,)), ((), ())), preferred_element_type=jnp.float32
                )
                scores[b, h] = product[h * group : (h + 1) * group] * scale
        return carry

    def value_chunk(c, carry):
        for i in range(CHUNK // per):
            block = c * (CHUNK // per) + i
            logs = jnp.zeros((group, width), jnp.float32)
            for k in range(per):
                logs = one_row(block * per + k, block, k, logs)
            sent[block, 2 * per * tile :] = split_logs(logs)
        return carry

    per_load = rows // LOADS // CHUNK
    small[0].wait()
    for which, chunk in ((0, score_chunk), (1, value_chunk)):
        if which:
            for copy in small[1:]:
                copy.wait()
        for c in range(LOADS):
            load(which, c).wait()
            lax.fori_loop(c * per_load, (c + 1) * per_load, chunk, 0)

    pl.semaphore_wait(barrier, 2 * half + outside.astype(jnp.int32))
    offsets = sorted((d for d in range(1 - half, half + 1) if d != 0), key=lambda d: -abs(d))
    for i, offset in enumerate(offsets):
        target = at(offset)
        remote(sent.at[lax.rem(target, WINDOW)], landed.at[i], a_send, a_recv, target).start()
    arrivals = pl.ds(0, len(offsets))
    first_copies = remote(sent.at[arrivals], landed.at[arrivals], a_send, a_recv, at(1))
    first_copies.wait_recv()

    mine = lax.rem(me, WINDOW)
    logs = [join_logs(sent[mine, 2 * per * tile :] if i < 0 else landed[i, 2 * per * tile :]) for i in range(-1, len(offsets))]
    top = functools.reduce(jnp.maximum, logs)
    shares = [jnp.exp(x - top) for x in logs]
    total = functools.reduce(jnp.add, shares)
    inverse = 1.0 / total
    merged = [jnp.zeros((group, width), jnp.float32) for _ in range(2 * per * heads)]
    for share, i in zip(shares, range(-1, len(offsets))):
        share = share * inverse
        for c in range(0, len(merged), heads):
            part = pl.ds(c * group, tile)
            values = (sent[mine, part] if i < 0 else landed[i, part]).astype(jnp.float32)
            for h in range(heads):
                merged[c + h] += column(share, c + h) * values[h * group : (h + 1) * group]
    for c in range(0, len(merged), heads):
        board[me, c * group : c * group + tile] = jnp.concatenate(merged[c : c + heads], axis=0).astype(jnp.bfloat16)
    board[me, 2 * per * tile :] = split_logs(jnp.where(lane < len(merged), top + jnp.log(total), 0.0))

    relays = n // STRIDE
    up = relays // 2 + 1
    split = relays // 4

    def spread(k):
        steps = [STRIDE] if k < up else []
        steps += [-(split + 1) * STRIDE] if k == split else []
        steps += [-STRIDE] if up + 1 < k else []
        copies = []
        for i, step in enumerate(([-1] if k else []) + steps + [1, 2]):
            target = (ROOT + k * STRIDE + step) % n
            copies.append(remote(out_ref, out_ref, c_send.at[i], c_recv, target))
            copies[-1].start()
        for copy in copies:
            copy.wait_send()

    @pl.when(me != root)
    def _():
        block = remote(board.at[me], board.at[me], b_send, b_recv, root)
        block.start()
        block.wait_send()
        remote(out_ref, out_ref, c_send.at[0], c_recv, root).wait_recv()
        for k in range(1, relays):

            @pl.when(me == (ROOT + k * STRIDE) % n)
            def _(k=k):
                spread(k)

    @pl.when(me == root)
    def _():
        gate_pad[...] = jnp.zeros_like(gate_pad)
        for branch in range(2):
            logits = gate_ref[branch]
            gate_pad[branch * rows : (branch + 1) * rows, : heads * group] = 1.0 / (1.0 + jnp.exp(-logits))
        turned = gate_pad[...].T
        for block in range(WINDOW):
            packed = jnp.zeros((group, width), jnp.float32)
            for k in range(per):
                for branch in range(2):
                    for h in range(heads):
                        c = (2 * k + branch) * heads + h
                        here = turned[h * group : (h + 1) * group]
                        moved = pltpu.roll(here, (c - (1 - branch) * rows - block * per - k) % width, 1)
                        packed = jnp.where(lane == c, moved, packed)
            gates[block] = packed

        others = pl.ds(0, n - 1)
        remote(board.at[others], board.at[others], b_send, b_recv, at(1)).wait_recv()
        early = []
        for block in range(WINDOW):
            logs = [join_logs(board[s * WINDOW + block, 2 * per * tile :]) for s in range(sources)]
            top = functools.reduce(jnp.maximum, logs)
            shares = [jnp.exp(x - top) for x in logs]
            inverse = 1.0 / functools.reduce(jnp.add, shares)
            factor = gates[block] * inverse
            shares = [x * factor for x in shares]
            for k in range(per):
                mixed = [jnp.zeros((group, width), jnp.float32) for _ in range(heads)]
                for s, share in enumerate(shares):
                    for branch in range(2):
                        c = (2 * k + branch) * heads
                        values = board[s * WINDOW + block, c * group : c * group + tile].astype(jnp.float32)
                        for h in range(heads):
                            mixed[h] += column(share, c + h) * values[h * group : (h + 1) * group]
                out_ref[block * per + k] = jnp.concatenate(mixed, axis=0).astype(jnp.bfloat16)
            if (block + 1) % (WINDOW // PARTS) == 0:
                part = pl.ds((block + 1 - WINDOW // PARTS) * per, rows // PARTS)
                send = c_send.at[5 + block // (WINDOW // PARTS)]
                early.append(remote(out_ref.at[part], out_ref.at[part], send, c_recv, (ROOT - 1) % n))
                early[-1].start()

        spread(0)
        for copy in early:
            copy.wait_send()

    first_copies.wait_send()


def on_device(n, queries, key_cache, value_cache, gate_logits, lengths, chosen, counts):
    rows, heads, context, width = key_cache.shape
    group = queries.shape[1] // heads
    lines = rows // WINDOW * 2 * heads * group + group
    vmem = pl.BlockSpec(memory_space=pltpu.VMEM)
    anywhere = pl.BlockSpec(memory_space=pl.ANY)
    return pl.pallas_call(
        functools.partial(kernel, n),
        name="decode",
        out_shape=pltpu.VMEM(queries.shape, jnp.bfloat16),
        in_specs=[anywhere] * 7,
        out_specs=vmem,
        scratch_shapes=[
            pltpu.VMEM(queries.shape, jnp.bfloat16),
            pltpu.VMEM(gate_logits.shape, jnp.float32),
            pltpu.SMEM(lengths.shape, jnp.int32),
            pltpu.VMEM(chosen.shape, jnp.int32),
            pltpu.SMEM((heads, rows), jnp.int32),
            pltpu.VMEM(key_cache.shape, jnp.bfloat16),
            pltpu.VMEM(value_cache.shape, jnp.bfloat16),
            pltpu.VMEM((WINDOW, lines, width), jnp.bfloat16),
            pltpu.VMEM((WINDOW - 1, lines, width), jnp.bfloat16),
            pltpu.VMEM((n, lines, width), jnp.bfloat16),
            pltpu.VMEM((width, width), jnp.float32),
            pltpu.VMEM((WINDOW, group, width), jnp.float32),
            pltpu.VMEM((rows, heads, group, context), jnp.float32),
            pltpu.SemaphoreType.DMA((5,)),
            pltpu.SemaphoreType.DMA((LOADS,)),
            pltpu.SemaphoreType.DMA((LOADS,)),
            pltpu.SemaphoreType.DMA,
            pltpu.SemaphoreType.DMA,
            pltpu.SemaphoreType.DMA,
            pltpu.SemaphoreType.DMA,
            pltpu.SemaphoreType.DMA((5 + PARTS,)),
            pltpu.SemaphoreType.DMA,
        ],
        compiler_params=pltpu.CompilerParams(collective_id=0, has_side_effects=True),
    )(queries, key_cache, value_cache, gate_logits, lengths, chosen, counts.T)


def solution(mesh):
    return jax.shard_map(
        functools.partial(on_device, mesh.shape["seq"]),
        mesh=mesh,
        in_specs=(
            P(("grp", "batch"), "head", None),
            P(("grp", "batch"), "head", "seq", None),
            P(("grp", "batch"), "head", "seq", None),
            P(None, ("grp", "batch"), "head"),
            P(("grp", "batch")),
            P(("grp", "batch"), "head", None),
            P(("grp", "batch"), "head"),
        ),
        out_specs=P(("grp", "batch"), "head", None),
        check_vma=False,
    )
```

```python
import functools
import math

import jax
import jax.numpy as jnp
from jax import lax
from jax.experimental import pallas as pl
from jax.experimental.pallas import tpu as pltpu
from jax.sharding import PartitionSpec as P

BLOCK = 128
WINDOW = 8
ROOT = 1
STRIDE = 4
PARTS = 4
CHUNK = 4
LOADS = 2
PIECE = 32
NEG = -1e30
MESH = pl.DeviceIdType.MESH


def iota(shape, dim):
    return lax.broadcasted_iota(jnp.int32, shape, dim)


def split_logs(logs):
    lane = iota(logs.shape, 1)
    spread = jnp.where(
        lane < PIECE,
        logs,
        jnp.where(lane < 2 * PIECE, pltpu.roll(logs, PIECE, 1), pltpu.roll(logs, 2 * PIECE, 1)),
    )
    high = spread.astype(jnp.bfloat16).astype(jnp.float32)
    rest = spread - high
    middle = rest.astype(jnp.bfloat16).astype(jnp.float32)
    low = rest - middle
    return jnp.where(lane < PIECE, high, jnp.where(lane < 2 * PIECE, middle, low)).astype(jnp.bfloat16)


def join_logs(pieces):
    pieces = pieces.astype(jnp.float32)
    width = pieces.shape[1]
    return (pieces + pltpu.roll(pieces, width - PIECE, 1)) + pltpu.roll(pieces, width - 2 * PIECE, 1)


def column(tile, lane):
    return jnp.broadcast_to(tile[:, lane : lane + 1], tile.shape)


def kernel(
    n,
    q_hbm,
    k_hbm,
    v_hbm,
    gate_hbm,
    length_hbm,
    chosen_hbm,
    count_hbm,
    out_ref,
    q_ref,
    gate_ref,
    length_ref,
    chosen_ref,
    count_ref,
    k_buf,
    v_buf,
    sent,
    landed,
    board,
    gate_pad,
    gates,
    scores,
    in_sem,
    k_sem,
    v_sem,
    a_send,
    a_recv,
    b_send,
    b_recv,
    c_send,
    c_recv,
):
    me = lax.axis_index("seq")
    rows, heads, context, width = k_buf.shape
    group = q_ref.shape[1] // heads
    local = context // BLOCK
    half = WINDOW // 2
    sources = n // WINDOW
    per = rows // WINDOW
    tile = heads * group
    scale = 1.0 / math.sqrt(width)

    def at(offset):
        return lax.rem(me + offset + n, n)

    def remote(src, dst, send, recv, target):
        return pltpu.make_async_remote_copy(
            src_ref=src,
            dst_ref=dst,
            send_sem=send,
            recv_sem=recv,
            device_id={"seq": target},
            device_id_type=MESH,
        )

    def load(which, c):
        part = pl.ds(c * (rows // LOADS), rows // LOADS)
        source, target, sem = (v_hbm, v_buf, v_sem) if which else (k_hbm, k_buf, k_sem)
        return pltpu.make_async_copy(source.at[part], target.at[part], sem.at[c])

    small = [
        pltpu.make_async_copy(source, target, in_sem.at[i])
        for i, (source, target) in enumerate(
            (
                (q_hbm, q_ref),
                (length_hbm, length_ref),
                (chosen_hbm, chosen_ref),
                (count_hbm, count_ref),
                (gate_hbm, gate_ref),
            )
        )
    ]
    small[0].start()
    for c in range(LOADS):
        for which in range(2):
            load(which, c).start()
        if c == 0:
            for copy in small[1:]:
                copy.start()

    root = ROOT
    away = lax.rem(root - me + n, n)
    outside = (away > half) & (away < n - half)
    barrier = pltpu.get_barrier_semaphore()
    for distance in range(half, 0, -1):
        for offset in (-distance, distance):
            pl.semaphore_signal(barrier, inc=1, device_id={"seq": at(offset)}, device_id_type=MESH)

    @pl.when(me == root)
    def _():
        for offset in range(half + 1, n - half):
            pl.semaphore_signal(barrier, inc=1, device_id={"seq": at(offset)}, device_id_type=MESH)

    lane = iota((group, width), 1)
    slot = iota((1, chosen_ref.shape[2]), 1)
    first = me * local

    def one_pair(b, h, live, root):
        parts = [scores[b, h, :, j * BLOCK : (j + 1) * BLOCK] for j in range(local)]
        chosen = chosen_ref[b, h : h + 1, :]
        listed = slot < count_ref[h, b]
        masks = []
        for j in range(local):
            hit = jnp.where((chosen == first + j) & listed, 1.0, 0.0)
            picked = jnp.max(hit, axis=1, keepdims=True)
            masks.append(live[j] & (jnp.broadcast_to(picked, (group, BLOCK)) > 0.5))
        kept = [jnp.where(m, s, NEG) for m, s in zip(masks, parts)]
        top = jnp.max(functools.reduce(jnp.maximum, kept), axis=1, keepdims=True)
        weights = [jnp.where(m, jnp.exp(s - top), 0.0) for m, s in zip(masks, kept)]
        total = jnp.sum(sum(weights), axis=1, keepdims=True)
        pooled = [
            jnp.where(
                live[j][:, :1],
                jnp.sum(jnp.where(live[j], parts[j], 0.0), axis=1, keepdims=True) * root[j],
                NEG,
            )
            for j in range(local)
        ]
        pool_top = functools.reduce(jnp.maximum, pooled)
        pool_weights = [jnp.where(live[j][:, :1], jnp.exp(pooled[j] - pool_top), 0.0) for j in range(local)]
        pool_total = sum(pool_weights)
        spread = [jnp.where(live[j], pool_weights[j] * root[j], 0.0) for j in range(local)]
        left = jnp.concatenate(
            [jnp.concatenate(weights, axis=1), jnp.concatenate(spread, axis=1)], axis=0
        ).astype(jnp.bfloat16)
        summed = jnp.dot(left, v_buf[b, h], preferred_element_type=jnp.float32)
        result = []
        for top_of, total_of, value in (
            (top, total, summed[:group]),
            (pool_top, pool_total, summed[group:]),
        ):
            some = total_of > 0.0
            safe = jnp.where(some, total_of, 1.0)
            result.append((value / safe, jnp.where(some, top_of + jnp.log(safe), NEG)))
        return result

    def one_row(b, block, k, logs):
        length = length_ref[b]
        live, root = [], []
        for j in range(local):
            start = (first + j) * BLOCK
            live.append(start + iota((group, BLOCK), 1) < length)
            filled = jnp.clip(length - start, 1, BLOCK).astype(jnp.float32)
            root.append(1.0 / jnp.sqrt(jnp.full((group, 1), filled, jnp.float32)))
        pairs = [one_pair(b, h, live, root) for h in range(heads)]
        for branch in range(2):
            values = jnp.concatenate([pairs[h][branch][0] for h in range(heads)], axis=0)
            sent[block, pl.ds((2 * k + branch) * tile, tile)] = values.astype(jnp.bfloat16)
            for h in range(heads):
                logs = jnp.where(lane == (2 * k + branch) * heads + h, pairs[h][branch][1], logs)
        return logs

    def score_chunk(c, carry):
        for i in range(CHUNK):
            b = c * CHUNK + i
            for h in range(heads):
                product = lax.dot_general(
                    q_ref[b], k_buf[b, h], (((1,), (1,)), ((), ())), preferred_element_type=jnp.float32
                )
                scores[b, h] = product[h * group : (h + 1) * group] * scale
        return carry

    def value_chunk(c, carry):
        for i in range(CHUNK // per):
            block = c * (CHUNK // per) + i
            logs = jnp.zeros((group, width), jnp.float32)
            for k in range(per):
                logs = one_row(block * per + k, block, k, logs)
            sent[block, 2 * per * tile :] = split_logs(logs)
        return carry

    per_load = rows // LOADS // CHUNK
    small[0].wait()
    for c in range(LOADS):
        load(0, c).wait()
        lax.fori_loop(c * per_load, (c + 1) * per_load, score_chunk, 0)
        if c == 0:
            for copy in small[1:]:
                copy.wait()
        load(1, c).wait()
        lax.fori_loop(c * per_load, (c + 1) * per_load, value_chunk, 0)

    pl.semaphore_wait(barrier, 2 * half + outside.astype(jnp.int32))
    offsets = sorted((d for d in range(1 - half, half + 1) if d != 0), key=lambda d: -abs(d))
    for i, offset in enumerate(offsets):
        target = at(offset)
        remote(sent.at[lax.rem(target, WINDOW)], landed.at[i], a_send, a_recv, target).start()
    arrivals = pl.ds(0, len(offsets))
    first_copies = remote(sent.at[arrivals], landed.at[arrivals], a_send, a_recv, at(1))
    first_copies.wait_recv()

    mine = lax.rem(me, WINDOW)
    logs = [join_logs(sent[mine, 2 * per * tile :] if i < 0 else landed[i, 2 * per * tile :]) for i in range(-1, len(offsets))]
    top = functools.reduce(jnp.maximum, logs)
    shares = [jnp.exp(x - top) for x in logs]
    total = functools.reduce(jnp.add, shares)
    inverse = 1.0 / total
    merged = [jnp.zeros((group, width), jnp.float32) for _ in range(2 * per * heads)]
    for share, i in zip(shares, range(-1, len(offsets))):
        share = share * inverse
        for c in range(0, len(merged), heads):
            part = pl.ds(c * group, tile)
            values = (sent[mine, part] if i < 0 else landed[i, part]).astype(jnp.float32)
            for h in range(heads):
                merged[c + h] += column(share, c + h) * values[h * group : (h + 1) * group]
    for c in range(0, len(merged), heads):
        board[me, c * group : c * group + tile] = jnp.concatenate(merged[c : c + heads], axis=0).astype(jnp.bfloat16)
    board[me, 2 * per * tile :] = split_logs(jnp.where(lane < len(merged), top + jnp.log(total), 0.0))

    relays = n // STRIDE
    up = relays // 2 + 1
    split = relays // 4

    def spread(k):
        steps = [STRIDE] if k < up else []
        steps += [-(split + 1) * STRIDE] if k == split else []
        steps += [-STRIDE] if up + 1 < k else []
        copies = []
        for i, step in enumerate([-1] + steps + [1, 2] if k else [1] + steps):
            target = (ROOT + k * STRIDE + step) % n
            copies.append(remote(out_ref, out_ref, c_send.at[i], c_recv, target))
            copies[-1].start()
        for copy in copies:
            copy.wait_send()

    @pl.when(me != root)
    def _():
        block = remote(board.at[me], board.at[me], b_send, b_recv, root)
        block.start()
        block.wait_send()
        remote(out_ref, out_ref, c_send.at[0], c_recv, root).wait_recv()
        second = remote(out_ref, out_ref, c_send.at[0], c_recv, (ROOT + 2) % n)

        @pl.when(me == (ROOT + 1) % n)
        def _():
            second.start()
            second.wait_send()

        for k in range(1, relays):

            @pl.when(me == (ROOT + k * STRIDE) % n)
            def _(k=k):
                spread(k)

    @pl.when(me == root)
    def _():
        gate_pad[...] = jnp.zeros_like(gate_pad)
        for branch in range(2):
            logits = gate_ref[branch]
            gate_pad[branch * rows : (branch + 1) * rows, : heads * group] = 1.0 / (1.0 + jnp.exp(-logits))
        turned = gate_pad[...].T
        for block in range(WINDOW):
            packed = jnp.zeros((group, width), jnp.float32)
            for k in range(per):
                for branch in range(2):
                    for h in range(heads):
                        c = (2 * k + branch) * heads + h
                        here = turned[h * group : (h + 1) * group]
                        moved = pltpu.roll(here, (c - (1 - branch) * rows - block * per - k) % width, 1)
                        packed = jnp.where(lane == c, moved, packed)
            gates[block] = packed

        others = pl.ds(0, n - 1)
        remote(board.at[others], board.at[others], b_send, b_recv, at(1)).wait_recv()
        early = []
        for block in range(WINDOW):
            logs = [join_logs(board[s * WINDOW + block, 2 * per * tile :]) for s in range(sources)]
            top = functools.reduce(jnp.maximum, logs)
            shares = [jnp.exp(x - top) for x in logs]
            inverse = 1.0 / functools.reduce(jnp.add, shares)
            factor = gates[block] * inverse
            shares = [x * factor for x in shares]
            for k in range(per):
                mixed = [jnp.zeros((group, width), jnp.float32) for _ in range(heads)]
                for s, share in enumerate(shares):
                    for branch in range(2):
                        c = (2 * k + branch) * heads
                        values = board[s * WINDOW + block, c * group : c * group + tile].astype(jnp.float32)
                        for h in range(heads):
                            mixed[h] += column(share, c + h) * values[h * group : (h + 1) * group]
                out_ref[block * per + k] = jnp.concatenate(mixed, axis=0).astype(jnp.bfloat16)
            if (block + 1) % (WINDOW // PARTS) == 0:
                part = pl.ds((block + 1 - WINDOW // PARTS) * per, rows // PARTS)
                send = c_send.at[5 + block // (WINDOW // PARTS)]
                early.append(remote(out_ref.at[part], out_ref.at[part], send, c_recv, (ROOT - 1) % n))
                early[-1].start()

        spread(0)
        for copy in early:
            copy.wait_send()

    first_copies.wait_send()


def on_device(n, queries, key_cache, value_cache, gate_logits, lengths, chosen, counts):
    rows, heads, context, width = key_cache.shape
    group = queries.shape[1] // heads
    lines = rows // WINDOW * 2 * heads * group + group
    vmem = pl.BlockSpec(memory_space=pltpu.VMEM)
    anywhere = pl.BlockSpec(memory_space=pl.ANY)
    return pl.pallas_call(
        functools.partial(kernel, n),
        name="decode",
        out_shape=pltpu.VMEM(queries.shape, jnp.bfloat16),
        in_specs=[anywhere] * 7,
        out_specs=vmem,
        scratch_shapes=[
            pltpu.VMEM(queries.shape, jnp.bfloat16),
            pltpu.VMEM(gate_logits.shape, jnp.float32),
            pltpu.SMEM(lengths.shape, jnp.int32),
            pltpu.VMEM(chosen.shape, jnp.int32),
            pltpu.SMEM((heads, rows), jnp.int32),
            pltpu.VMEM(key_cache.shape, jnp.bfloat16),
            pltpu.VMEM(value_cache.shape, jnp.bfloat16),
            pltpu.VMEM((WINDOW, lines, width), jnp.bfloat16),
            pltpu.VMEM((WINDOW - 1, lines, width), jnp.bfloat16),
            pltpu.VMEM((n, lines, width), jnp.bfloat16),
            pltpu.VMEM((width, width), jnp.float32),
            pltpu.VMEM((WINDOW, group, width), jnp.float32),
            pltpu.VMEM((rows, heads, group, context), jnp.float32),
            pltpu.SemaphoreType.DMA((5,)),
            pltpu.SemaphoreType.DMA((LOADS,)),
            pltpu.SemaphoreType.DMA((LOADS,)),
            pltpu.SemaphoreType.DMA,
            pltpu.SemaphoreType.DMA,
            pltpu.SemaphoreType.DMA,
            pltpu.SemaphoreType.DMA,
            pltpu.SemaphoreType.DMA((5 + PARTS,)),
            pltpu.SemaphoreType.DMA,
        ],
        compiler_params=pltpu.CompilerParams(collective_id=0, has_side_effects=True),
    )(queries, key_cache, value_cache, gate_logits, lengths, chosen, counts.T)


def solution(mesh):
    return jax.shard_map(
        functools.partial(on_device, mesh.shape["seq"]),
        mesh=mesh,
        in_specs=(
            P(("grp", "batch"), "head", None),
            P(("grp", "batch"), "head", "seq", None),
            P(("grp", "batch"), "head", "seq", None),
            P(None, ("grp", "batch"), "head"),
            P(("grp", "batch")),
            P(("grp", "batch"), "head", None),
            P(("grp", "batch"), "head"),
        ),
        out_specs=P(("grp", "batch"), "head", None),
        check_vma=False,
    )
```
